16 devices in a mesh: dp: 2 (over y, z), tp: 8 (over x, core).
Axes of the slice: x: 4, y: 2, z: 1, core: 2. Of those that a mesh axis runs over, the one named last changes fastest.
The devices are a block of a 4x4x8 slice.
Arguments:
- tokens: bfloat16 [8, 2048, 2048], P('dp'), parts along dimension 0
- seq_lens: int32 [8], P('dp'), parts along dimension 0
- w_q: bfloat16 [2048, 2048], P(None, 'tp')
- w_k: bfloat16 [2048, 2048], P(None, 'tp')
- w_v: bfloat16 [2048, 2048], P(None, 'tp')
- w_o: bfloat16 [2048, 2048], P('tp')
- g_q: bfloat16 [2048], P('tp')
- g_k: bfloat16 [2048], P('tp')
- g_attn: bfloat16 [2048], replicated
- g_mlp: bfloat16 [2048], replicated
- w_gate: bfloat16 [2048, 8192], P(None, 'tp')
- w_up: bfloat16 [2048, 8192], P(None, 'tp')
- w_down: bfloat16 [8192, 2048], P('tp')
Outputs:
- output 1: bfloat16 [8, 2048, 2048], P('dp'), parts along dimension 0
- output 2: bfloat16 [8, 16, 2048, 128], P('dp', 'tp'), parts along dimension 0
- output 3: bfloat16 [8, 16, 2048, 128], P('dp', 'tp'), parts along dimension 0
There are 2 independent parts. The reference program is written for one: setup_inputs(seed, part) draws one part's arguments, and reference() takes and returns one part's arrays. A program takes and returns all parts, laid end to end along the dimension named above; an argument that names none is the same for every part.
All inputs are finite; a program needn't handle non-finite values.
Results may differ from the reference program's by a relative error of at most 0.0182036.
Values are sent between devices in bfloat16 or wider.
A program may use at most 768 MiB of HBM per device.

```python
import jax
import jax.numpy as jnp
from jax import lax

PROMPTS = 4
SEQ_LEN = 2048
D_MODEL = 2048
Q_HEADS = 16
KV_HEADS = 16
HEAD_DIM = 128
FF_DIM = 8192

ROPE_BASE = 500000.0
NORM_EPS = 1e-6


def setup_inputs(seed: int = 0, part: int = 0) -> dict:
    part_key = jax.random.fold_in(jax.random.key(seed), part)
    key_tok, key_len, key_slot = jax.random.split(part_key, 3)
    weight_keys = jax.random.split(jax.random.key(seed + 1), 13)
    q_width = Q_HEADS * HEAD_DIM
    kv_width = KV_HEADS * HEAD_DIM
    in_scale = D_MODEL ** -0.5
    tokens = jax.random.normal(key_tok, (PROMPTS, SEQ_LEN, D_MODEL), jnp.float32)
    seq_lens = jax.random.randint(key_len, (PROMPTS,), SEQ_LEN // 8, SEQ_LEN + 1, jnp.int32)
    full_slot = jax.random.randint(key_slot, (), 0, PROMPTS, jnp.int32)
    seq_lens = jnp.where(jnp.arange(PROMPTS) == full_slot, SEQ_LEN, seq_lens).astype(jnp.int32)
    q_head_scale = 2.0 ** jax.random.uniform(weight_keys[0], (Q_HEADS, 1), jnp.float32, -1.0, 1.0)
    k_head_scale = 2.0 ** jax.random.uniform(weight_keys[1], (KV_HEADS, 1), jnp.float32, -1.0, 1.0)
    w_q = (jax.random.normal(weight_keys[2], (D_MODEL, Q_HEADS, HEAD_DIM), jnp.float32) * q_head_scale * in_scale).reshape(D_MODEL, q_width)
    w_k = (jax.random.normal(weight_keys[3], (D_MODEL, KV_HEADS, HEAD_DIM), jnp.float32) * k_head_scale * in_scale).reshape(D_MODEL, kv_width)
    w_v = jax.random.normal(weight_keys[4], (D_MODEL, kv_width), jnp.float32) * in_scale
    w_o = jax.random.normal(weight_keys[5], (q_width, D_MODEL), jnp.float32) * q_width ** -0.5
    g_q = jax.random.uniform(weight_keys[6], (q_width,), jnp.float32, 0.5, 1.5)
    g_k = jax.random.uniform(weight_keys[7], (kv_width,), jnp.float32, 0.5, 1.5)
    g_attn = jax.random.uniform(weight_keys[8], (D_MODEL,), jnp.float32, 0.5, 1.5)
    g_mlp = jax.random.uniform(weight_keys[9], (D_MODEL,), jnp.float32, 0.5, 1.5)
    w_gate = jax.random.normal(weight_keys[10], (D_MODEL, FF_DIM), jnp.float32) * in_scale
    w_up = jax.random.normal(weight_keys[11], (D_MODEL, FF_DIM), jnp.float32) * in_scale
    w_down = jax.random.normal(weight_keys[12], (FF_DIM, D_MODEL), jnp.float32) * FF_DIM ** -0.5
    return dict(tokens=tokens.astype(jnp.bfloat16), seq_lens=seq_lens, w_q=w_q.astype(jnp.bfloat16), w_k=w_k.astype(jnp.bfloat16), w_v=w_v.astype(jnp.bfloat16), w_o=w_o.astype(jnp.bfloat16), g_q=g_q.astype(jnp.bfloat16), g_k=g_k.astype(jnp.bfloat16), g_attn=g_attn.astype(jnp.bfloat16), g_mlp=g_mlp.astype(jnp.bfloat16), w_gate=w_gate.astype(jnp.bfloat16), w_up=w_up.astype(jnp.bfloat16), w_down=w_down.astype(jnp.bfloat16))


def rope_tables(seq_len, head_dim):
    half_dim = head_dim // 2
    inv_freq = ROPE_BASE ** (-2.0 * jnp.arange(half_dim, dtype=jnp.float32) / head_dim)
    angles = jnp.arange(seq_len, dtype=jnp.float32)[:, None] * inv_freq[None, :]
    angles = jnp.concatenate([angles, angles], axis=-1)
    return jnp.cos(angles), jnp.sin(angles)


def apply_rope(vecs, cos_tab, sin_tab, head_axes):
    half_dim = vecs.shape[-1] // 2
    table_shape = (cos_tab.shape[0],) + (1,) * head_axes + (cos_tab.shape[1],)
    rotated = jnp.concatenate([-vecs[..., half_dim:], vecs[..., :half_dim]], axis=-1)
    return vecs * cos_tab.reshape(table_shape) + rotated * sin_tab.reshape(table_shape)


def rms_scale(vals):
    return lax.rsqrt(jnp.mean(vals * vals, axis=-1, keepdims=True) + NORM_EPS)


def post_norm(base, branch, gain):
    branch32 = branch.astype(jnp.float32)
    return (base.astype(jnp.float32) + branch32 * rms_scale(branch32) * gain.astype(jnp.float32)).astype(jnp.bfloat16)


def reference(tokens, seq_lens, w_q, w_k, w_v, w_o, g_q, g_k, g_attn, g_mlp, w_gate, w_up, w_down):
    group_size = Q_HEADS // KV_HEADS
    cos_tab, sin_tab = rope_tables(SEQ_LEN, HEAD_DIM)
    positions = jnp.arange(SEQ_LEN)
    causal = positions[None, :] <= positions[:, None]

    def one_prompt(item):
        prompt, length = item
        q_raw = jnp.dot(prompt, w_q, preferred_element_type=jnp.float32)
        k_raw = jnp.dot(prompt, w_k, preferred_element_type=jnp.float32)
        v_new = jnp.dot(prompt, w_v, preferred_element_type=jnp.float32).astype(jnp.bfloat16)
        q_norm = q_raw * rms_scale(q_raw) * g_q.astype(jnp.float32)
        k_norm = k_raw * rms_scale(k_raw) * g_k.astype(jnp.float32)
        queries = apply_rope(q_norm.reshape(SEQ_LEN, KV_HEADS, group_size, HEAD_DIM), cos_tab, sin_tab, 2).astype(jnp.bfloat16)
        keys_new = apply_rope(k_norm.reshape(SEQ_LEN, KV_HEADS, HEAD_DIM), cos_tab, sin_tab, 1).astype(jnp.bfloat16)
        v_heads = v_new.reshape(SEQ_LEN, KV_HEADS, HEAD_DIM)
        scores = jnp.einsum('sgrd,tgd->grst', queries.astype(jnp.float32), keys_new.astype(jnp.float32)) * HEAD_DIM ** -0.5
        allowed = causal & (positions[None, :] < length)
        scores = jnp.where(allowed, scores, -1e30)
        attn_probs = jax.nn.softmax(scores, axis=-1).astype(jnp.bfloat16)
        attn_out = jnp.einsum('grst,tgd->sgrd', attn_probs.astype(jnp.float32), v_heads.astype(jnp.float32)).astype(jnp.bfloat16)
        attn_proj = jnp.dot(attn_out.reshape(SEQ_LEN, Q_HEADS * HEAD_DIM), w_o, preferred_element_type=jnp.float32).astype(jnp.bfloat16)
        hidden = post_norm(prompt, attn_proj, g_attn)
        gate_pre = jnp.dot(hidden, w_gate, preferred_element_type=jnp.float32)
        up_proj = jnp.dot(hidden, w_up, preferred_element_type=jnp.float32)
        act_out = (jax.nn.silu(gate_pre) * up_proj).astype(jnp.bfloat16)
        mlp_out = jnp.dot(act_out, w_down, preferred_element_type=jnp.float32).astype(jnp.bfloat16)
        new_hidden = post_norm(hidden, mlp_out, g_mlp)
        return new_hidden, jnp.transpose(keys_new, (1, 0, 2)), jnp.transpose(v_heads, (1, 0, 2))

    out_hidden, k_cache, v_cache = lax.map(one_prompt, (tokens, seq_lens))
    return out_hidden, k_cache, v_cache
```

```python
import functools
import math

import jax
import jax.numpy as jnp
from jax import lax
from jax.experimental import pallas as pl
from jax.experimental.pallas import tpu as pltpu
from jax.sharding import PartitionSpec as P

HEAD_DIM = 128
ROPE_BASE = 500000.0
NORM_EPS = 1e-6
ROWS = 512
F32 = jnp.float32
BF16 = jnp.bfloat16
MESH = pl.DeviceIdType.MESH
VMEM_BYTES = 67_000_000


def rope_tables(seq_len, head_dim):
    half_dim = head_dim // 2
    inv_freq = ROPE_BASE ** (-2.0 * jnp.arange(half_dim, dtype=F32) / head_dim)
    angles = jnp.arange(seq_len, dtype=F32)[:, None] * inv_freq[None, :]
    sin = jnp.sin(angles)
    cos = jnp.cos(angles)
    return jnp.concatenate([cos, cos], axis=-1), jnp.concatenate([-sin, sin], axis=-1)


def send(src, dst, send_sem, recv_sem, peer):
    pltpu.make_async_remote_copy(src_ref=src, dst_ref=dst, send_sem=send_sem, recv_sem=recv_sem, device_id={'tp': peer}, device_id_type=MESH).start()


def wait_for(ref, sem):
    pltpu.make_async_copy(ref, ref, sem).wait()


def neighbours(tp_size):
    me = lax.axis_index('tp')
    chips = tp_size // 2
    chip, core = me // 2, me % 2
    right = ((chip + 1) % chips) * 2 + core
    left = ((chip + chips - 1) % chips) * 2 + core
    return me, chip, core, right, left, chip * 2 + 1 - core


def qkv_kernel(x_ref, wq_ref, wk_ref, wv_ref, q_ref, k_ref, v_ref, ss_ref):
    x = x_ref[...]
    q = jnp.dot(x, wq_ref[...], preferred_element_type=F32)
    k = jnp.dot(x, wk_ref[...], preferred_element_type=F32)
    v = jnp.dot(x, wv_ref[...], preferred_element_type=F32).astype(BF16)
    q_ref[...] = q
    k_ref[...] = k
    for h in range(v_ref.shape[1]):
        v_ref[0, h] = v[:, h * HEAD_DIM:(h + 1) * HEAD_DIM]
    qs = jnp.sum(q * q, axis=-1, keepdims=True)
    ks = jnp.sum(k * k, axis=-1, keepdims=True)
    lane = lax.broadcasted_iota(jnp.int32, (q.shape[0], 128), 1)
    t = jnp.transpose(jnp.where(lane < 64, qs, ks))
    ss_ref[0:1] = t[0:1]
    ss_ref[1:2] = t[64:65]


def qkv(x, w_q, w_k, w_v, prompts):
    total, d = x.shape
    n = w_q.shape[1]
    heads = n // HEAD_DIM
    seq = total // prompts
    per = seq // ROWS
    whole = lambda a: pl.BlockSpec(a.shape, lambda i: (0, 0))
    return pl.pallas_call(
        qkv_kernel,
        grid=(total // ROWS,),
        in_specs=[pl.BlockSpec((ROWS, d), lambda i: (i, 0)), whole(w_q), whole(w_k), whole(w_v)],
        out_specs=[
            pl.BlockSpec((ROWS, n), lambda i: (i, 0)),
            pl.BlockSpec((ROWS, n), lambda i: (i, 0)),
            pl.BlockSpec((1, heads, ROWS, HEAD_DIM), lambda i: (i // per, 0, i % per, 0)),
            pl.BlockSpec((2, ROWS), lambda i: (0, i)),
        ],
        out_shape=[
            jax.ShapeDtypeStruct((total, n), F32),
            jax.ShapeDtypeStruct((total, n), F32),
            jax.ShapeDtypeStruct((prompts, heads, seq, HEAD_DIM), BF16),
            jax.ShapeDtypeStruct((2, total), F32),
        ],
        cost_estimate=pl.CostEstimate(flops=2 * total * d * n * 3, bytes_accessed=2 * total * d + 10 * total * n, transcendentals=0),
        name="qkv",
    )(x, w_q, w_k, w_v)


PASS, PASS2, USE, SLOTS = 2, 3, 4, 8


def attn_kernel(lens_ref, q_ref, k_ref, v_ref, ss_ref, cos_ref, sin_ref, gq_ref, gk_ref, wo_ref, x_ref, ga_ref, h_ref, kc_ref,
                k_s, o_buf, ss_all, ss_send, ss_recv, got_l, got_r, half_l, half_r, got_s, sent, free_l, free_r, free_s,
                *, tp_size, chunks, blocks, width):
    s = pl.program_id(0)
    me, chip, core, right, left, sib = neighbours(tp_size)
    rows, n = q_ref.shape
    heads = kc_ref.shape[1]
    mid = rows // 2

    def cols(dev):
        return pl.ds(pl.multiple_of(dev * n, n), n)

    @pl.when(s == 0)
    def _():
        barrier = pltpu.get_barrier_semaphore()
        for d in range(1, tp_size):
            pl.semaphore_signal(barrier, inc=1, device_id={'tp': (me + d) % tp_size}, device_id_type=MESH)
        pl.semaphore_wait(barrier, tp_size - 1)
        for d in range(1, tp_size):
            send(ss_ref, ss_all.at[me], ss_send.at[d], ss_recv.at[me], (me + d) % tp_size)
        ss_all[pl.ds(me, 1)] = ss_ref[...][None]
        for d in range(1, tp_size):
            peer = (me + d) % tp_size
            wait_for(ss_all.at[peer], ss_recv.at[peer])
            wait_for(ss_ref, ss_send.at[d])

    @pl.when((s >= PASS) & (s < chunks + PASS))
    def _():
        slot = (s - PASS) % SLOTS
        buf = o_buf.at[slot]
        wait_for(buf.at[:, cols(left)], got_l.at[slot])
        first = buf.at[pl.ds(0, mid), cols(left)]
        send(first, first, sent.at[slot], half_l.at[slot], right)
        send(buf.at[:, cols(left)], buf.at[:, cols(left)], sent.at[slot], got_s.at[slot], sib)
        wait_for(buf.at[:, cols(right)], got_r.at[slot])
        second = buf.at[pl.ds(mid, mid), cols(right)]
        send(second, second, sent.at[slot], half_r.at[slot], left)
        send(buf.at[:, cols(right)], buf.at[:, cols(right)], sent.at[slot], got_s.at[slot], sib)

    @pl.when(s < chunks)
    def _():
        ss = jnp.sum(ss_all[:, :, pl.ds(pl.multiple_of(s * rows, rows), rows)], axis=0)
        scale = lax.rsqrt(ss / width + NORM_EPS)
        col_scale = jnp.transpose(jnp.concatenate([scale, jnp.zeros((6, rows), F32)], axis=0))
        cos, sin = cos_ref[...], sin_ref[...]

        def rope(t):
            return (t * cos + pltpu.roll(t, HEAD_DIM // 2, axis=1) * sin).astype(BF16)

        i = s % blocks
        b = s // blocks
        length = lens_ref[b]
        slot = s % SLOTS
        qn = q_ref[...] * col_scale[:, 0:1] * gq_ref[...]
        kn = k_ref[...] * col_scale[:, 1:2] * gk_ref[...]
        qh = []
        for h in range(heads):
            sl = slice(h * HEAD_DIM, (h + 1) * HEAD_DIM)
            kr = rope(kn[:, sl])
            kc_ref[0, h] = kr
            k_s[h, pl.ds(pl.multiple_of(i * rows, rows), rows), :] = kr
            qh.append(rope(qn[:, sl]))
        c = HEAD_DIM ** -0.5 * math.log2(math.e)
        for j in range(blocks):
            @pl.when(i == j)
            def _():
                kv = (j + 1) * rows
                col = lax.broadcasted_iota(jnp.int32, (1, kv), 1)
                bias = jnp.where(col < length, 0.0, -1e30).astype(F32)
                r = lax.broadcasted_iota(jnp.int32, (rows, rows), 0)
                cc = lax.broadcasted_iota(jnp.int32, (rows, rows), 1)
                tri = jnp.where(cc <= r, 0.0, -1e30).astype(F32)
                for h in range(heads):
                    sc = lax.dot_general(qh[h], k_s[h, 0:kv, :], (((1,), (1,)), ((), ())), preferred_element_type=F32)
                    sc = sc + bias
                    diag = sc[:, j * rows:] + tri
                    sc = diag if j == 0 else jnp.concatenate([sc[:, :j * rows], diag], axis=1)
                    m = jnp.max(sc, axis=-1, keepdims=True)
                    e = jnp.exp2(sc * c - m * c)
                    p = (e * (1.0 / jnp.sum(e, axis=-1, keepdims=True))).astype(BF16)
                    o = jnp.dot(p, v_ref[0, h, 0:kv, :], preferred_element_type=F32)
                    o_buf[slot, :, pl.ds(pl.multiple_of(me * n + h * HEAD_DIM, HEAD_DIM), HEAD_DIM)] = o.astype(BF16)

    @pl.when((s >= PASS2) & (s < chunks + PASS2))
    def _():
        slot = (s - PASS2) % SLOTS
        buf = o_buf.at[slot]
        far = ((chip + 2) % (tp_size // 2)) * 2 + core
        first = buf.at[pl.ds(0, mid), cols(far)]
        second = buf.at[pl.ds(mid, mid), cols(far)]
        wait_for(first, half_l.at[slot])
        send(first, first, sent.at[slot], got_s.at[slot], sib)
        wait_for(second, half_r.at[slot])
        send(second, second, sent.at[slot], got_s.at[slot], sib)

    @pl.when((s >= USE) & (s < chunks + USE))
    def _():
        t = s - USE
        slot = t % SLOTS
        buf = o_buf.at[slot]
        wait_for(buf.at[:, pl.ds(0, 4 * n)], got_s.at[slot])
        wait_for(buf.at[:, pl.ds(0, 7 * n)], sent.at[slot])
        d = h_ref.shape[1]
        step = 512
        sq = jnp.zeros((rows, 1), F32)
        for lo in range(0, d, step):
            a = jnp.dot(o_buf[slot], wo_ref[:, lo:lo + step], preferred_element_type=F32).astype(BF16)
            h_ref[:, lo:lo + step] = a
            a = a.astype(F32)
            sq = sq + jnp.sum(a * a, axis=-1, keepdims=True)
        scale = lax.rsqrt(sq / d + NORM_EPS)
        for lo in range(0, d, step):
            a = h_ref[:, lo:lo + step].astype(F32)
            h_ref[:, lo:lo + step] = (x_ref[:, lo:lo + step].astype(F32) + a * scale * ga_ref[:, lo:lo + step]).astype(BF16)

        @pl.when(t < chunks - SLOTS)
        def _():
            for sem, peer in ((free_r, left), (free_l, right), (free_s, sib)):
                pl.semaphore_signal(sem, inc=1, device_id={'tp': peer}, device_id_type=MESH)

    @pl.when(s < chunks)
    def _():
        slot = s % SLOTS

        @pl.when(s >= SLOTS)
        def _():
            for sem in (free_r, free_l, free_s):
                pl.semaphore_wait(sem, 1)

        own = o_buf.at[slot, :, cols(me)]
        send(own, own, sent.at[slot], got_l.at[slot], right)
        send(own, own, sent.at[slot], got_r.at[slot], left)
        send(own, own, sent.at[slot], got_s.at[slot], sib)


def attend(q, k, v, ss, cos, sin, g_q, g_k, lens, w_o, x, g_attn, tp_size):
    prompts, heads, seq, _ = v.shape
    n = heads * HEAD_DIM
    total, d = x.shape
    blocks = seq // ROWS
    chunks = total // ROWS
    now = lambda s: jnp.minimum(s, chunks - 1)
    used = lambda s: jnp.clip(s - USE, 0, chunks - 1)
    vmem = pl.BlockSpec(memory_space=pltpu.VMEM)
    dma = pltpu.SemaphoreType.DMA
    return pl.pallas_call(
        functools.partial(attn_kernel, tp_size=tp_size, chunks=chunks, blocks=blocks, width=n * tp_size),
        grid=(chunks + USE,),
        in_specs=[
            pl.BlockSpec(memory_space=pltpu.SMEM),
            pl.BlockSpec((ROWS, n), lambda s: (now(s), 0)),
            pl.BlockSpec((ROWS, n), lambda s: (now(s), 0)),
            pl.BlockSpec((1, heads, seq, HEAD_DIM), lambda s: (now(s) // blocks, 0, 0, 0)),
            vmem,
            pl.BlockSpec((ROWS, HEAD_DIM), lambda s: (now(s) % blocks, 0)),
            pl.BlockSpec((ROWS, HEAD_DIM), lambda s: (now(s) % blocks, 0)),
            vmem, vmem, vmem,
            pl.BlockSpec((ROWS, d), lambda s: (used(s), 0)),
            vmem,
        ],
        out_specs=[
            pl.BlockSpec((ROWS, d), lambda s: (used(s), 0)),
            pl.BlockSpec((1, heads, ROWS, HEAD_DIM), lambda s: (now(s) // blocks, 0, now(s) % blocks, 0)),
        ],
        out_shape=[
            jax.ShapeDtypeStruct((total, d), BF16),
            jax.ShapeDtypeStruct((prompts, heads, seq, HEAD_DIM), BF16),
        ],
        scratch_shapes=[
            pltpu.VMEM((heads, seq, HEAD_DIM), BF16),
            pltpu.VMEM((SLOTS, ROWS, n * tp_size), BF16),
            pltpu.VMEM((tp_size,) + ss.shape, F32),
            dma((tp_size,)), dma((tp_size,)),
            dma((SLOTS,)), dma((SLOTS,)), dma((SLOTS,)), dma((SLOTS,)), dma((SLOTS,)), dma((SLOTS,)),
            pltpu.SemaphoreType.REGULAR, pltpu.SemaphoreType.REGULAR, pltpu.SemaphoreType.REGULAR,
        ],
        compiler_params=pltpu.CompilerParams(collective_id=1, has_side_effects=True, vmem_limit_bytes=VMEM_BYTES),
        cost_estimate=pl.CostEstimate(flops=2 * total * d * n * tp_size, bytes_accessed=4 * total * d, transcendentals=0),
        name="attend",
    )(lens, q, k, v, ss, cos, sin, g_q, g_k, w_o, x, g_attn)


ADD, MERGE, FINAL, RELAY, RELAY2, DONE = 1, 3, 5, 7, 9, 10
SIB_SLOTS = 3


def mlp_kernel(h_ref, wg_ref, wu_ref, wd_ref, gm_ref, y_ref, act_s, m_s, c_s, r_sib, r1_l, r1_r, r2_l, r2_r, h_own, y_own,
               sib_send, sib_recv, s1_send, r1_lsem, r1_rsem, s2_send, r2_lsem, r2_rsem,
               y_send, y_loc, y_l, y_r, yh_l, yh_r, yf_send, yh_send, y_sib, free_s, *, tp_size, chunks):
    s = pl.program_id(0)
    me, chip, core, right, left, sib = neighbours(tp_size)
    chips = tp_size // 2
    rows, d = h_ref.shape
    half = rows // 2
    piece = half // chips
    sub = piece // 2
    opp = (chip + 2) % chips
    rchip = (chip + 1) % chips
    lchip = (chip + chips - 1) % chips
    own = pl.ds(pl.multiple_of(core * half, half), half)
    other = pl.ds(pl.multiple_of((1 - core) * half, half), half)

    def at(p, off=0, size=piece):
        return pl.ds(pl.multiple_of(p * piece + off, sub), size)

    def y_rows(t, c, p, off=0, size=piece):
        return y_ref.at[pl.ds(pl.multiple_of(t * rows + c * half + p * piece + off, sub), size)]

    def stage(lag):
        return pl.when((s >= lag) & (s < chunks + lag))

    @pl.when(s == 0)
    def _():
        barrier = pltpu.get_barrier_semaphore()
        for peer in (right, left, sib):
            pl.semaphore_signal(barrier, inc=1, device_id={'tp': peer}, device_id_type=MESH)
        pl.semaphore_wait(barrier, 3)

    @stage(0)
    def _():
        f = act_s.shape[1]
        h = h_ref[...]
        for lo in range(0, f, 512):
            gate = jnp.dot(h, wg_ref[:, lo:lo + 512], preferred_element_type=F32)
            up = jnp.dot(h, wu_ref[:, lo:lo + 512], preferred_element_type=F32)
            act_s[:, lo:lo + 512] = (jax.nn.silu(gate) * up).astype(BF16)
        act = act_s[...]
        for lo in range(0, d, 512):
            m_s[s % SIB_SLOTS, :, lo:lo + 512] = jnp.dot(act, wd_ref[:, lo:lo + 512], preferred_element_type=F32).astype(BF16)
        h_own[s % 8] = h_ref[pl.ds(pl.multiple_of(core * half + chip * piece, piece), piece), :]

    @stage(ADD)
    def _():
        t = s - ADD
        slot, ms = t % 8, t % SIB_SLOTS
        wait_for(r_sib.at[ms], sib_recv.at[ms])
        wait_for(m_s.at[ms, other], sib_send.at[ms])
        c_s[slot] = (m_s[ms, own, :].astype(F32) + r_sib[ms].astype(F32)).astype(BF16)

        @pl.when(t < chunks - SIB_SLOTS)
        def _():
            pl.semaphore_signal(free_s, inc=1, device_id={'tp': sib}, device_id_type=MESH)

    @stage(MERGE)
    def _():
        slot = (s - MERGE) % 8
        wait_for(r1_l.at[slot], r1_lsem.at[slot])
        c_s[slot, at(rchip, 0, sub), :] = (c_s[slot, at(rchip, 0, sub), :].astype(F32) + r1_l[slot].astype(F32)).astype(BF16)
        wait_for(r1_r.at[slot], r1_rsem.at[slot])
        c_s[slot, at(lchip, sub, sub), :] = (c_s[slot, at(lchip, sub, sub), :].astype(F32) + r1_r[slot].astype(F32)).astype(BF16)

    @stage(FINAL)
    def _():
        t = s - FINAL
        slot = t % 8
        wait_for(r2_l.at[slot], r2_lsem.at[slot])
        wait_for(r2_r.at[slot], r2_rsem.at[slot])
        wait_for(c_s.at[slot, pl.ds(0, piece)], s1_send.at[slot])
        wait_for(c_s.at[slot, pl.ds(0, 2 * piece)], s2_send.at[slot])
        m = c_s[slot, at(chip), :].astype(F32) + r2_l[slot].astype(F32) + r2_r[slot].astype(F32)
        m = m.astype(BF16).astype(F32)
        scale = lax.rsqrt(jnp.sum(m * m, axis=-1, keepdims=True) / d + NORM_EPS)
        y_own[slot] = (h_own[slot].astype(F32) + m * scale * gm_ref[...]).astype(BF16)

    @stage(RELAY)
    def _():
        t = s - RELAY
        slot = t % 8
        from_l, from_r = y_rows(t, core, lchip), y_rows(t, core, rchip)
        wait_for(from_l, y_l.at[slot])
        first = y_rows(t, core, lchip, 0, sub)
        send(first, first, yf_send.at[slot], yh_l.at[slot], right)
        send(from_l, from_l, yf_send.at[slot], y_sib.at[t], sib)
        wait_for(from_r, y_r.at[slot])
        second = y_rows(t, core, rchip, sub, sub)
        send(second, second, yf_send.at[slot], yh_r.at[slot], left)
        send(from_r, from_r, yf_send.at[slot], y_sib.at[t], sib)

    @stage(RELAY2)
    def _():
        t = s - RELAY2
        slot = t % 8
        first, second = y_rows(t, core, opp, 0, sub), y_rows(t, core, opp, sub, sub)
        wait_for(first, yh_l.at[slot])
        send(first, first, yh_send.at[slot], y_sib.at[t], sib)
        wait_for(second, yh_r.at[slot])
        send(second, second, yh_send.at[slot], y_sib.at[t], sib)

    @stage(DONE)
    def _():
        t = s - DONE
        slot = t % 8
        base = pl.multiple_of(t * rows, rows)
        wait_for(y_ref.at[pl.ds(base, piece)], y_loc.at[slot])
        wait_for(y_ref.at[pl.ds(base, 3 * piece)], y_send.at[slot])
        wait_for(y_ref.at[pl.ds(base, 3 * piece)], yf_send.at[slot])
        wait_for(y_ref.at[pl.ds(base, piece)], yh_send.at[slot])
        wait_for(y_ref.at[pl.ds(base, chips * piece)], y_sib.at[t])

    @stage(FINAL)
    def _():
        t = s - FINAL
        slot = t % 8
        dst = y_rows(t, core, chip)
        send(y_own.at[slot], dst, y_send.at[slot], y_l.at[slot], right)
        send(y_own.at[slot], dst, y_send.at[slot], y_r.at[slot], left)
        send(y_own.at[slot], dst, y_send.at[slot], y_sib.at[t], sib)
        pltpu.make_async_copy(y_own.at[slot], dst, y_loc.at[slot]).start()

    @stage(MERGE)
    def _():
        slot = (s - MERGE) % 8
        send(c_s.at[slot, at(rchip)], r2_l.at[slot], s2_send.at[slot], r2_lsem.at[slot], right)
        send(c_s.at[slot, at(lchip)], r2_r.at[slot], s2_send.at[slot], r2_rsem.at[slot], left)

    @stage(ADD)
    def _():
        slot = (s - ADD) % 8
        send(c_s.at[slot, at(opp, 0, sub)], r1_l.at[slot], s1_send.at[slot], r1_lsem.at[slot], right)
        send(c_s.at[slot, at(opp, sub, sub)], r1_r.at[slot], s1_send.at[slot], r1_rsem.at[slot], left)

    @stage(0)
    def _():
        @pl.when(s >= SIB_SLOTS)
        def _():
            pl.semaphore_wait(free_s, 1)

        ms = s % SIB_SLOTS
        send(m_s.at[ms, other], r_sib.at[ms], sib_send.at[ms], sib_recv.at[ms], sib)


def mlp(h, w_gate, w_up, w_down, g_mlp, tp_size):
    total, d = h.shape
    f = w_gate.shape[1]
    chunks = total // ROWS
    half = ROWS // 2
    piece = half // (tp_size // 2)
    sub = piece // 2
    vmem = pl.BlockSpec(memory_space=pltpu.VMEM)
    dma = pltpu.SemaphoreType.DMA
    return pl.pallas_call(
        functools.partial(mlp_kernel, tp_size=tp_size, chunks=chunks),
        grid=(chunks + DONE,),
        in_specs=[pl.BlockSpec((ROWS, d), lambda s: (jnp.minimum(s, chunks - 1), 0)), vmem, vmem, vmem, vmem],
        out_specs=pl.BlockSpec(memory_space=pl.ANY),
        out_shape=jax.ShapeDtypeStruct((total, d), BF16),
        scratch_shapes=[
            pltpu.VMEM((ROWS, f), BF16),
            pltpu.VMEM((SIB_SLOTS, ROWS, d), BF16),
            pltpu.VMEM((8, half, d), BF16),
            pltpu.VMEM((SIB_SLOTS, half, d), BF16),
            pltpu.VMEM((8, sub, d), BF16), pltpu.VMEM((8, sub, d), BF16),
            pltpu.VMEM((8, piece, d), BF16), pltpu.VMEM((8, piece, d), BF16),
            pltpu.VMEM((8, piece, d), BF16), pltpu.VMEM((8, piece, d), BF16),
            dma((SIB_SLOTS,)), dma((SIB_SLOTS,)),
            dma((8,)), dma((8,)), dma((8,)), dma((8,)), dma((8,)), dma((8,)),
            dma((8,)), dma((8,)), dma((8,)), dma((8,)), dma((8,)), dma((8,)), dma((8,)), dma((8,)),
            dma((chunks,)),
            pltpu.SemaphoreType.REGULAR,
        ],
        compiler_params=pltpu.CompilerParams(collective_id=2, has_side_effects=True, vmem_limit_bytes=VMEM_BYTES),
        cost_estimate=pl.CostEstimate(flops=6 * total * d * f, bytes_accessed=4 * total * d, transcendentals=0),
        name="mlp",
    )(h, w_gate, w_up, w_down, g_mlp)


def solution(mesh):
    tp_size = mesh.shape['tp']

    def local_layer(tokens, seq_lens, w_q, w_k, w_v, w_o, g_q, g_k, g_attn, g_mlp, w_gate, w_up, w_down):
        prompts, seq, d = tokens.shape
        x = tokens.reshape(prompts * seq, d)
        w_o_full = lax.all_gather(w_o, 'tp', axis=0, tiled=True)
        q, k, v_cache, ss = qkv(x, w_q, w_k, w_v, prompts)
        cos, sin = rope_tables(seq, HEAD_DIM)
        row = lambda g: g.astype(F32)[None]
        h, k_cache = attend(q, k, v_cache, ss, cos, sin, row(g_q), row(g_k), seq_lens, w_o_full, x, row(g_attn), tp_size)
        y = mlp(h, w_gate, w_up, w_down, row(g_mlp), tp_size)
        return y.reshape(prompts, seq, d), k_cache, v_cache

    return jax.shard_map(local_layer, mesh=mesh, in_specs=(P('dp', None, None), P('dp'), P(None, 'tp'), P(None, 'tp'), P(None, 'tp'), P('tp', None), P('tp'), P('tp'), P(), P(), P(None, 'tp'), P(None, 'tp'), P('tp', None)), out_specs=(P('dp', None, None), P('dp', 'tp', None, None), P('dp', 'tp', None, None)), check_vma=False)
```

```python
import functools
import math

import jax
import jax.numpy as jnp
import numpy as np
from jax import lax
from jax.experimental import pallas as pl
from jax.experimental.pallas import tpu as pltpu
from jax.sharding import PartitionSpec as P

HEAD_DIM = 128
ROPE_BASE = 500000.0
NORM_EPS = 1e-6
ROWS = 512
MLP_ROWS = 256
LATE = 4
F32 = jnp.float32
BF16 = jnp.bfloat16
MESH = pl.DeviceIdType.MESH
VMEM_BYTES = 67_000_000


def rope_tables(rows, blocks, head_dim):
    half = head_dim // 2
    inv_freq = np.tile(ROPE_BASE ** (-2.0 * np.arange(half) / head_dim), 2)
    fine = np.arange(rows)[:, None] * inv_freq[None]
    coarse = np.arange(blocks)[:, None] * rows * inv_freq[None]
    return [f(a).astype(np.float32) for a in (fine, coarse) for f in (np.cos, np.sin)]


def send(src, dst, send_sem, recv_sem, peer):
    pltpu.make_async_remote_copy(src_ref=src, dst_ref=dst, send_sem=send_sem, recv_sem=recv_sem, device_id={'tp': peer}, device_id_type=MESH).start()


def wait_for(ref, sem):
    pltpu.make_async_copy(ref, ref, sem).wait()


def neighbours(tp_size):
    me = lax.axis_index('tp')
    chips = tp_size // 2
    chip, core = me // 2, me % 2
    right = ((chip + 1) % chips) * 2 + core
    left = ((chip + chips - 1) % chips) * 2 + core
    return me, chip, core, right, left, chip * 2 + 1 - core


ATT, PASS, PASS2, DONE1 = 2, 4, 5, 6
SUM_SLOTS, QK_SLOTS, WO_PIECES, WO_PASS, WO_PASS2 = 4, 3, 4, 5, 8


def attn_kernel(lens_ref, x_ref, wq_ref, wk_ref, wv_ref, g_ref, fcos_ref, fsin_ref, ccos_ref, csin_ref, wo_ref,
                o_ref, o_late, wo_all, kc_ref, vc_ref,
                q_s, k_s, kr_s, v_s, o_own, ss_own, ss_all, ss_send, ss_recv, o_send, o_loc, got_l, got_r, half_l, half_r, got_s, late_loc,
                pass_send, pass2_send, wo_send, wo_loc, wo_l, wo_r, wo_hl, wo_hr, wo_s, *, tp_size, chunks, blocks, width):
    s = pl.program_id(0)
    me, chip, core, right, left, sib = neighbours(tp_size)
    far = ((chip + 2) % (tp_size // 2)) * 2 + core
    rows = x_ref.shape[0]
    n = wq_ref.shape[1]
    heads = kc_ref.shape[1]
    mid = rows // 2
    wo_rows = wo_ref.shape[0]
    gathered = chunks - LATE

    def o_at(t, dev, off=0, size=rows):
        return o_ref.at[pl.ds(pl.multiple_of(t * rows + off, mid), size), pl.ds(pl.multiple_of(dev * n, n), n)]

    def wo_at(dev, off=0, size=wo_rows):
        return wo_all.at[pl.ds(pl.multiple_of(dev * wo_rows + off, wo_rows // WO_PIECES), size)]

    def stage(lag, count=chunks):
        return pl.when((s >= lag) & (s < count + lag))

    @pl.when(s == 0)
    def _():
        barrier = pltpu.get_barrier_semaphore()
        for d in range(1, tp_size):
            pl.semaphore_signal(barrier, inc=1, device_id={'tp': (me + d) % tp_size}, device_id_type=MESH)
        pl.semaphore_wait(barrier, tp_size - 1)
        pltpu.make_async_copy(wo_ref, wo_at(me), wo_loc).start()

    @stage(PASS + LATE, gathered)
    def _():
        t = s - PASS - LATE
        slot = t % 8
        from_l, from_r = o_at(t, left), o_at(t, right)
        wait_for(from_l, got_l.at[slot])
        first = o_at(t, left, 0, mid)
        send(first, first, pass_send.at[slot], half_l.at[slot], right)
        send(from_l, from_l, pass_send.at[slot], got_s.at[slot], sib)
        wait_for(from_r, got_r.at[slot])
        second = o_at(t, right, mid, mid)
        send(second, second, pass_send.at[slot], half_r.at[slot], left)
        send(from_r, from_r, pass_send.at[slot], got_s.at[slot], sib)

    @stage(0)
    def _():
        x = x_ref[...]
        slot = s % QK_SLOTS
        b = (s // blocks) % 2
        here = pl.ds(pl.multiple_of((s % blocks) * rows, rows), rows)
        q = jnp.dot(x, wq_ref[...], preferred_element_type=F32)
        q_s[slot] = q
        k = jnp.dot(x, wk_ref[...], preferred_element_type=F32)
        k_s[slot] = k
        v = jnp.dot(x, wv_ref[...], preferred_element_type=F32).astype(BF16)
        for h in range(heads):
            vh = v[:, h * HEAD_DIM:(h + 1) * HEAD_DIM]
            vc_ref[0, h] = vh
            v_s[b, h, here, :] = vh
        qs = jnp.sum(q * q, axis=-1, keepdims=True)
        ks = jnp.sum(k * k, axis=-1, keepdims=True)
        lane = lax.broadcasted_iota(jnp.int32, (rows, 128), 1)
        t = jnp.transpose(jnp.where(lane < 64, qs, ks))
        ss_own[s % SUM_SLOTS] = jnp.concatenate([t[0:1], t[64:65]], axis=0)

    @stage(ATT)
    def _():
        t = s - ATT
        sslot = t % SUM_SLOTS
        for d in range(1, tp_size):
            peer = (me + d) % tp_size
            wait_for(ss_all.at[sslot, peer], ss_recv.at[sslot, peer])
        wait_for(ss_all.at[sslot, pl.ds(0, tp_size - 1)], ss_send.at[sslot])
        ss = ss_own[sslot]
        for d in range(1, tp_size):
            ss = ss + ss_all[sslot, (me + d) % tp_size]
        scale = lax.rsqrt(ss / width + NORM_EPS)
        col_scale = jnp.transpose(jnp.concatenate([scale, jnp.zeros((6, rows), F32)], axis=0))
        i = t % blocks
        b = t // blocks
        slot = t % 8
        lane = lax.broadcasted_iota(jnp.int32, (1, HEAD_DIM), 1)
        ccos, csin = ccos_ref[pl.ds(i, 1), :], csin_ref[pl.ds(i, 1), :]
        cos = fcos_ref[...] * ccos - fsin_ref[...] * csin
        sin = (fsin_ref[...] * ccos + fcos_ref[...] * csin) * jnp.where(lane < HEAD_DIM // 2, -1.0, 1.0)

        def rope(u):
            return (u * cos + pltpu.roll(u, HEAD_DIM // 2, axis=1) * sin).astype(BF16)

        length = lens_ref[b]
        qn = q_s[t % QK_SLOTS] * col_scale[:, 0:1] * g_ref[:, 0:n]
        kn = k_s[t % QK_SLOTS] * col_scale[:, 1:2] * g_ref[:, n:2 * n]
        qh = []
        for h in range(heads):
            sl = slice(h * HEAD_DIM, (h + 1) * HEAD_DIM)
            kr = rope(kn[:, sl])
            kc_ref[0, h] = kr
            kr_s[h, pl.ds(pl.multiple_of(i * rows, rows), rows), :] = kr
            qh.append(rope(qn[:, sl]))
        c = HEAD_DIM ** -0.5 * math.log2(math.e)
        for j in range(blocks):
            @pl.when(i == j)
            def _():
                kv = (j + 1) * rows
                col = lax.broadcasted_iota(jnp.int32, (1, kv), 1)
                bias = jnp.where(col < length, 0.0, -1e30).astype(F32)
                r = lax.broadcasted_iota(jnp.int32, (rows, rows), 0)
                cc = lax.broadcasted_iota(jnp.int32, (rows, rows), 1)
                tri = jnp.where(cc <= r, 0.0, -1e30).astype(F32)
                for h in range(heads):
                    sc = lax.dot_general(qh[h], kr_s[h, 0:kv, :], (((1,), (1,)), ((), ())), preferred_element_type=F32)
                    sc = sc + bias
                    diag = sc[:, j * rows:] + tri
                    sc = diag if j == 0 else jnp.concatenate([sc[:, :j * rows], diag], axis=1)
                    m = jnp.max(sc, axis=-1, keepdims=True)
                    e = jnp.exp2(sc * c - m * c)
                    p = (e * (1.0 / jnp.sum(e, axis=-1, keepdims=True))).astype(BF16)
                    o = jnp.dot(p, v_s[b % 2, h, 0:kv, :], preferred_element_type=F32)
                    o_own[slot, :, h * HEAD_DIM:(h + 1) * HEAD_DIM] = o.astype(BF16)

    @stage(PASS2 + LATE, gathered)
    def _():
        t = s - PASS2 - LATE
        slot = t % 8
        first, second = o_at(t, far, 0, mid), o_at(t, far, mid, mid)
        wait_for(first, half_l.at[slot])
        send(first, first, pass2_send.at[slot], got_s.at[slot], sib)
        wait_for(second, half_r.at[slot])
        send(second, second, pass2_send.at[slot], got_s.at[slot], sib)

    @stage(DONE1 + LATE, gathered)
    def _():
        t = s - DONE1 - LATE
        slot = t % 8
        part = o_ref.at[pl.ds(pl.multiple_of(t * rows, rows), rows)]
        wait_for(part.at[:, pl.ds(0, 3 * n)], o_send.at[slot])
        wait_for(part.at[:, pl.ds(0, n)], o_loc.at[slot])
        wait_for(part.at[:, pl.ds(0, 3 * n)], pass_send.at[slot])
        wait_for(part.at[:, pl.ds(0, n)], pass2_send.at[slot])
        wait_for(part.at[:, pl.ds(0, 4 * n)], got_s.at[slot])

    @stage(0)
    def _():
        slot = s % SUM_SLOTS
        for d in range(1, tp_size):
            send(ss_own.at[slot], ss_all.at[slot, me], ss_send.at[slot], ss_recv.at[slot, me], (me + d) % tp_size)

    @stage(ATT, LATE)
    def _():
        t = s - ATT
        pltpu.make_async_copy(o_own.at[t % 8], o_late.at[pl.ds(pl.multiple_of(t * rows, rows), rows)], late_loc.at[t]).start()

    @stage(DONE1, LATE)
    def _():
        t = s - DONE1
        wait_for(o_own.at[t % 8], late_loc.at[t])

    @stage(ATT + LATE, gathered)
    def _():
        t = s - ATT - LATE
        slot = t % 8
        own = o_own.at[(t + LATE) % 8]
        send(own, o_at(t, me), o_send.at[slot], got_l.at[slot], right)
        send(own, o_at(t, me), o_send.at[slot], got_r.at[slot], left)
        send(own, o_at(t, me), o_send.at[slot], got_s.at[slot], sib)
        pltpu.make_async_copy(own, o_at(t, me), o_loc.at[slot]).start()

    @pl.when(s < WO_PIECES)
    def _():
        size = wo_rows // WO_PIECES
        piece = wo_ref.at[pl.ds(pl.multiple_of(s * size, size), size)]
        send(piece, wo_at(me, s * size, size), wo_send, wo_l, right)
        send(piece, wo_at(me, s * size, size), wo_send, wo_r, left)
        send(piece, wo_at(me, s * size, size), wo_send, wo_s, sib)

    @pl.when(s == WO_PASS)
    def _():
        size = wo_rows // 2
        wait_for(wo_at(left), wo_l)
        send(wo_at(left, 0, size), wo_at(left, 0, size), wo_send, wo_hl, right)
        send(wo_at(left), wo_at(left), wo_send, wo_s, sib)
        wait_for(wo_at(right), wo_r)
        send(wo_at(right, size, size), wo_at(right, size, size), wo_send, wo_hr, left)
        send(wo_at(right), wo_at(right), wo_send, wo_s, sib)

    @pl.when(s == WO_PASS2)
    def _():
        size = wo_rows // 2
        wait_for(wo_at(far, 0, size), wo_hl)
        send(wo_at(far, 0, size), wo_at(far, 0, size), wo_send, wo_s, sib)
        wait_for(wo_at(far, size, size), wo_hr)
        send(wo_at(far, size, size), wo_at(far, size, size), wo_send, wo_s, sib)

    @pl.when(s == chunks + DONE1 - 1)
    def _():
        wait_for(wo_ref, wo_loc)
        wait_for(wo_all.at[pl.ds(0, 7 * wo_rows)], wo_send)
        wait_for(wo_all.at[pl.ds(0, 4 * wo_rows)], wo_s)


def attend(x, prompts, w_q, w_k, w_v, gains, lens, w_o, tp_size):
    total, d = x.shape
    n = w_q.shape[1]
    heads = n // HEAD_DIM
    seq = total // prompts
    blocks = seq // ROWS
    chunks = total // ROWS
    now = lambda s: jnp.minimum(s, chunks - 1)
    att = lambda s: jnp.clip(s - ATT, 0, chunks - 1)
    vmem = pl.BlockSpec(memory_space=pltpu.VMEM)
    hbm = pl.BlockSpec(memory_space=pl.ANY)
    dma = pltpu.SemaphoreType.DMA
    cache = jax.ShapeDtypeStruct((prompts, heads, seq, HEAD_DIM), BF16)
    tables = [jnp.asarray(t) for t in rope_tables(ROWS, blocks, HEAD_DIM)]
    return pl.pallas_call(
        functools.partial(attn_kernel, tp_size=tp_size, chunks=chunks, blocks=blocks, width=n * tp_size),
        grid=(chunks + DONE1,),
        in_specs=[
            pl.BlockSpec(memory_space=pltpu.SMEM),
            pl.BlockSpec((ROWS, d), lambda s: (now(s), 0)),
            vmem, vmem, vmem, vmem, vmem, vmem, vmem, vmem, hbm,
        ],
        out_specs=[
            hbm, hbm, hbm,
            pl.BlockSpec((1, heads, ROWS, HEAD_DIM), lambda s: (att(s) // blocks, 0, att(s) % blocks, 0)),
            pl.BlockSpec((1, heads, ROWS, HEAD_DIM), lambda s: (now(s) // blocks, 0, now(s) % blocks, 0)),
        ],
        out_shape=[
            jax.ShapeDtypeStruct((total - LATE * ROWS, n * tp_size), BF16),
            jax.ShapeDtypeStruct((LATE * ROWS, n), BF16),
            jax.ShapeDtypeStruct((w_o.shape[0] * tp_size, w_o.shape[1]), BF16),
            cache, cache,
        ],
        scratch_shapes=[
            pltpu.VMEM((QK_SLOTS, ROWS, n), F32),
            pltpu.VMEM((QK_SLOTS, ROWS, n), F32),
            pltpu.VMEM((heads, seq, HEAD_DIM), BF16),
            pltpu.VMEM((2, heads, seq, HEAD_DIM), BF16),
            pltpu.VMEM((8, ROWS, n), BF16),
            pltpu.VMEM((SUM_SLOTS, 2, ROWS), F32),
            pltpu.VMEM((SUM_SLOTS, tp_size, 2, ROWS), F32),
            dma((SUM_SLOTS,)), dma((SUM_SLOTS, tp_size)),
            dma((8,)), dma((8,)), dma((8,)), dma((8,)), dma((8,)), dma((8,)), dma((8,)), dma((LATE,)), dma((8,)), dma((8,)),
            dma, dma, dma, dma, dma, dma, dma,
        ],
        compiler_params=pltpu.CompilerParams(collective_id=1, has_side_effects=True, vmem_limit_bytes=VMEM_BYTES),
        cost_estimate=pl.CostEstimate(flops=6 * total * d * n, bytes_accessed=4 * total * d, transcendentals=0),
        name="attend",
    )(lens, x, w_q, w_k, w_v, gains, *tables, w_o)


ADD, MERGE, FINAL, RELAY, RELAY2, DONE = 1, 3, 5, 7, 9, 10
LATE_PASS, LATE_PASS2, LATE_DONE = 4, 7, 14
SIB_SLOTS, C_SLOTS = 3, 6


def mlp_kernel(o_ref, late_ref, x_ref, wo_ref, g_ref, wg_ref, wu_ref, wd_ref, y_ref, o_late, o_s, h_ref, act_s, m_s, c_s, r_sib, r1_l, r1_r, r2_l, r2_r, h_own, y_own,
               sib_send, sib_recv, s1_send, r1_lsem, r1_rsem, s2_send, r2_lsem, r2_rsem,
               y_send, y_loc, y_l, y_r, yh_l, yh_r, yf_send, yh_send, y_sib, free_s, late_send, late_loc, late_l, late_r, late_hl, late_hr, late_s, *, tp_size, chunks, early):
    s = pl.program_id(0)
    me, chip, core, right, left, sib = neighbours(tp_size)
    chips = tp_size // 2
    rows, d = x_ref.shape
    n, late_mid = late_ref.shape[1], late_ref.shape[0] // 2
    g_at = g_ref.shape[1] - 2 * d
    half = rows // 2
    piece = half // chips
    sub = piece // 2
    opp = (chip + 2) % chips
    rchip = (chip + 1) % chips
    lchip = (chip + chips - 1) % chips
    own = pl.ds(pl.multiple_of(core * half, half), half)
    other = pl.ds(pl.multiple_of((1 - core) * half, half), half)

    def at(p, off=0, size=piece):
        return pl.ds(pl.multiple_of(p * piece + off, sub), size)

    def y_rows(t, c, p, off=0, size=piece):
        return y_ref.at[pl.ds(pl.multiple_of((t + chunks - early) % chunks * rows + c * half + p * piece + off, sub), size)]

    def late(dev, off=0, size=2 * late_mid):
        return o_late.at[pl.ds(off, size), pl.ds(pl.multiple_of(dev * n, n), n)]

    def stage(lag):
        return pl.when((s >= lag) & (s < chunks + lag))

    @pl.when(s == 0)
    def _():
        barrier = pltpu.get_barrier_semaphore()
        for peer in (right, left, sib):
            pl.semaphore_signal(barrier, inc=1, device_id={'tp': peer}, device_id_type=MESH)
        pl.semaphore_wait(barrier, 3)
        for peer, sem in ((right, late_l), (left, late_r), (sib, late_s)):
            send(late_ref, late(me), late_send, sem, peer)
        pltpu.make_async_copy(late_ref, late(me), late_loc).start()

    @pl.when(s == LATE_PASS)
    def _():
        wait_for(late(left), late_l)
        send(late(left, 0, late_mid), late(left, 0, late_mid), late_send, late_hl, right)
        send(late(left), late(left), late_send, late_s, sib)
        wait_for(late(right), late_r)
        send(late(right, late_mid, late_mid), late(right, late_mid, late_mid), late_send, late_hr, left)
        send(late(right), late(right), late_send, late_s, sib)

    @pl.when(s == LATE_PASS2)
    def _():
        far = opp * 2 + core
        wait_for(late(far, 0, late_mid), late_hl)
        send(late(far, 0, late_mid), late(far, 0, late_mid), late_send, late_s, sib)
        wait_for(late(far, late_mid, late_mid), late_hr)
        send(late(far, late_mid, late_mid), late(far, late_mid, late_mid), late_send, late_s, sib)

    @pl.when(s == LATE_DONE)
    def _():
        wait_for(late_ref, late_loc)
        wait_for(o_late.at[:, pl.ds(0, 7 * n)], late_send)
        wait_for(o_late.at[:, pl.ds(0, 4 * n)], late_s)

    @pl.when(s < early)
    def _():
        o_s[...] = o_ref[...]

    @pl.when((s >= early) & (s < chunks))
    def _():
        o_s[...] = o_late[pl.ds(pl.multiple_of((s - early) * rows, rows), rows), :]

    @stage(0)
    def _():
        f = act_s.shape[1]
        o = o_s[...]
        sq = jnp.zeros((rows, 1), F32)
        for lo in range(0, d, 512):
            a = jnp.dot(o, wo_ref[:, lo:lo + 512], preferred_element_type=F32).astype(BF16)
            h_ref[:, lo:lo + 512] = a
            a = a.astype(F32)
            sq = sq + jnp.sum(a * a, axis=-1, keepdims=True)
        scale = lax.rsqrt(sq / d + NORM_EPS)
        for lo in range(0, d, 512):
            a = h_ref[:, lo:lo + 512].astype(F32)
            h_ref[:, lo:lo + 512] = (x_ref[:, lo:lo + 512].astype(F32) + a * scale * g_ref[:, g_at + lo:g_at + lo + 512]).astype(BF16)
        h = h_ref[...]
        for lo in range(0, f, 512):
            gate = jnp.dot(h, wg_ref[:, lo:lo + 512], preferred_element_type=F32)
            up = jnp.dot(h, wu_ref[:, lo:lo + 512], preferred_element_type=F32)
            act_s[:, lo:lo + 512] = (jax.nn.silu(gate) * up).astype(BF16)
        act = act_s[...]
        for lo in range(0, d, 512):
            m_s[s % SIB_SLOTS, :, lo:lo + 512] = jnp.dot(act, wd_ref[:, lo:lo + 512], preferred_element_type=F32).astype(BF16)
        h_own[s % 8] = h_ref[pl.ds(pl.multiple_of(core * half + chip * piece, piece), piece), :]

    @stage(ADD)
    def _():
        t = s - ADD
        slot, ms, cs = t % 8, t % SIB_SLOTS, t % C_SLOTS
        wait_for(r_sib.at[ms], sib_recv.at[ms])
        wait_for(m_s.at[ms, other], sib_send.at[ms])
        c_s[cs] = (m_s[ms, own, :].astype(F32) + r_sib[ms].astype(F32)).astype(BF16)

        @pl.when(t < chunks - SIB_SLOTS)
        def _():
            pl.semaphore_signal(free_s, inc=1, device_id={'tp': sib}, device_id_type=MESH)

    @stage(MERGE)
    def _():
        slot, cs = (s - MERGE) % 8, (s - MERGE) % C_SLOTS
        wait_for(r1_l.at[slot], r1_lsem.at[slot])
        c_s[cs, at(rchip, 0, sub), :] = (c_s[cs, at(rchip, 0, sub), :].astype(F32) + r1_l[slot].astype(F32)).astype(BF16)
        wait_for(r1_r.at[slot], r1_rsem.at[slot])
        c_s[cs, at(lchip, sub, sub), :] = (c_s[cs, at(lchip, sub, sub), :].astype(F32) + r1_r[slot].astype(F32)).astype(BF16)

    @stage(FINAL)
    def _():
        t = s - FINAL
        slot, cs = t % 8, t % C_SLOTS
        wait_for(r2_l.at[slot], r2_lsem.at[slot])
        wait_for(r2_r.at[slot], r2_rsem.at[slot])
        wait_for(c_s.at[cs, pl.ds(0, piece)], s1_send.at[slot])
        wait_for(c_s.at[cs, pl.ds(0, 2 * piece)], s2_send.at[slot])
        m = c_s[cs, at(chip), :].astype(F32) + r2_l[slot].astype(F32) + r2_r[slot].astype(F32)
        m = m.astype(BF16).astype(F32)
        scale = lax.rsqrt(jnp.sum(m * m, axis=-1, keepdims=True) / d + NORM_EPS)
        y_own[slot] = (h_own[slot].astype(F32) + m * scale * g_ref[:, g_at + d:]).astype(BF16)

    @stage(RELAY)
    def _():
        t = s - RELAY
        slot = t % 8
        from_l, from_r = y_rows(t, core, lchip), y_rows(t, core, rchip)
        wait_for(from_l, y_l.at[slot])
        first = y_rows(t, core, lchip, 0, sub)
        send(first, first, yf_send.at[slot], yh_l.at[slot], right)
        send(from_l, from_l, yf_send.at[slot], y_sib.at[t], sib)
        wait_for(from_r, y_r.at[slot])
        second = y_rows(t, core, rchip, sub, sub)
        send(second, second, yf_send.at[slot], yh_r.at[slot], left)
        send(from_r, from_r, yf_send.at[slot], y_sib.at[t], sib)

    @stage(RELAY2)
    def _():
        t = s - RELAY2
        slot = t % 8
        first, second = y_rows(t, core, opp, 0, sub), y_rows(t, core, opp, sub, sub)
        wait_for(first, yh_l.at[slot])
        send(first, first, yh_send.at[slot], y_sib.at[t], sib)
        wait_for(second, yh_r.at[slot])
        send(second, second, yh_send.at[slot], y_sib.at[t], sib)

    @stage(DONE)
    def _():
        t = s - DONE
        slot = t % 8
        base = pl.multiple_of(t * rows, rows)
        wait_for(y_ref.at[pl.ds(base, piece)], y_loc.at[slot])
        wait_for(y_ref.at[pl.ds(base, 3 * piece)], y_send.at[slot])
        wait_for(y_ref.at[pl.ds(base, 3 * piece)], yf_send.at[slot])
        wait_for(y_ref.at[pl.ds(base, piece)], yh_send.at[slot])
        wait_for(y_ref.at[pl.ds(base, chips * piece)], y_sib.at[t])

    @stage(FINAL)
    def _():
        t = s - FINAL
        slot = t % 8
        dst = y_rows(t, core, chip)
        send(y_own.at[slot], dst, y_send.at[slot], y_l.at[slot], right)
        send(y_own.at[slot], dst, y_send.at[slot], y_r.at[slot], left)
        send(y_own.at[slot], dst, y_send.at[slot], y_sib.at[t], sib)
        pltpu.make_async_copy(y_own.at[slot], dst, y_loc.at[slot]).start()

    @stage(MERGE)
    def _():
        slot, cs = (s - MERGE) % 8, (s - MERGE) % C_SLOTS
        send(c_s.at[cs, at(rchip)], r2_l.at[slot], s2_send.at[slot], r2_lsem.at[slot], right)
        send(c_s.at[cs, at(lchip)], r2_r.at[slot], s2_send.at[slot], r2_rsem.at[slot], left)

    @stage(ADD)
    def _():
        slot, cs = (s - ADD) % 8, (s - ADD) % C_SLOTS
        send(c_s.at[cs, at(opp, 0, sub)], r1_l.at[slot], s1_send.at[slot], r1_lsem.at[slot], right)
        send(c_s.at[cs, at(opp, sub, sub)], r1_r.at[slot], s1_send.at[slot], r1_rsem.at[slot], left)

    @stage(0)
    def _():
        @pl.when(s >= SIB_SLOTS)
        def _():
            pl.semaphore_wait(free_s, 1)

        ms = s % SIB_SLOTS
        send(m_s.at[ms, other], r_sib.at[ms], sib_send.at[ms], sib_recv.at[ms], sib)


def mlp(o, late, x, w_o, gains, w_gate, w_up, w_down, tp_size):
    total, d = x.shape
    f = w_gate.shape[1]
    chunks = total // MLP_ROWS
    half = MLP_ROWS // 2
    piece = half // (tp_size // 2)
    sub = piece // 2
    early = o.shape[0] // MLP_ROWS
    front = pl.BlockSpec((MLP_ROWS, d), lambda s: (jnp.minimum(s, early - 1), 0))
    chunk = pl.BlockSpec((MLP_ROWS, d), lambda s: ((jnp.minimum(s, chunks - 1) + chunks - early) % chunks, 0))
    vmem = pl.BlockSpec(memory_space=pltpu.VMEM)
    dma = pltpu.SemaphoreType.DMA
    return pl.pallas_call(
        functools.partial(mlp_kernel, tp_size=tp_size, chunks=chunks, early=early),
        grid=(chunks + DONE,),
        in_specs=[front, pl.BlockSpec(memory_space=pl.ANY), chunk, vmem, vmem, vmem, vmem, vmem],
        out_specs=pl.BlockSpec(memory_space=pl.ANY),
        out_shape=jax.ShapeDtypeStruct((total, d), BF16),
        scratch_shapes=[
            pltpu.VMEM((late.shape[0], d), BF16),
            pltpu.VMEM((MLP_ROWS, d), BF16),
            pltpu.VMEM((MLP_ROWS, d), BF16),
            pltpu.VMEM((MLP_ROWS, f), BF16),
            pltpu.VMEM((SIB_SLOTS, MLP_ROWS, d), BF16),
            pltpu.VMEM((C_SLOTS, half, d), BF16),
            pltpu.VMEM((SIB_SLOTS, half, d), BF16),
            pltpu.VMEM((8, sub, d), BF16), pltpu.VMEM((8, sub, d), BF16),
            pltpu.VMEM((8, piece, d), BF16), pltpu.VMEM((8, piece, d), BF16),
            pltpu.VMEM((8, piece, d), BF16), pltpu.VMEM((8, piece, d), BF16),
            dma((SIB_SLOTS,)), dma((SIB_SLOTS,)),
            dma((8,)), dma((8,)), dma((8,)), dma((8,)), dma((8,)), dma((8,)),
            dma((8,)), dma((8,)), dma((8,)), dma((8,)), dma((8,)), dma((8,)), dma((8,)), dma((8,)),
            dma((chunks,)),
            pltpu.SemaphoreType.REGULAR,
            dma, dma, dma, dma, dma, dma, dma,
        ],
        compiler_params=pltpu.CompilerParams(collective_id=2, has_side_effects=True, vmem_limit_bytes=VMEM_BYTES),
        cost_estimate=pl.CostEstimate(flops=6 * total * d * f + 2 * total * d * d, bytes_accessed=4 * total * d, transcendentals=0),
        name="mlp",
    )(o, late, x, w_o, gains, w_gate, w_up, w_down)


def solution(mesh):
    tp_size = mesh.shape['tp']

    def local_layer(tokens, seq_lens, w_q, w_k, w_v, w_o, g_q, g_k, g_attn, g_mlp, w_gate, w_up, w_down):
        prompts, seq, d = tokens.shape
        x = tokens.reshape(prompts * seq, d)
        gains = jnp.concatenate([g_q, g_k, g_attn, g_mlp]).astype(F32)[None]
        o, o_late, w_o_full, k_cache, v_cache = attend(x, prompts, w_q, w_k, w_v, gains, seq_lens, w_o, tp_size)
        y = mlp(o, o_late, x, w_o_full, gains, w_gate, w_up, w_down, tp_size)
        return y.reshape(prompts, seq, d), k_cache, v_cache

    return jax.shard_map(local_layer, mesh=mesh, in_specs=(P('dp', None, None), P('dp'), P(None, 'tp'), P(None, 'tp'), P(None, 'tp'), P('tp', None), P('tp'), P('tp'), P(), P(), P(None, 'tp'), P(None, 'tp'), P('tp', None)), out_specs=(P('dp', None, None), P('dp', 'tp', None, None), P('dp', 'tp', None, None)), check_vma=False)
```

```python
import functools
import math

import jax
import jax.numpy as jnp
import numpy as np
from jax import lax
from jax.experimental import pallas as pl
from jax.experimental.pallas import tpu as pltpu
from jax.sharding import PartitionSpec as P

HEAD_DIM = 128
ROPE_BASE = 500000.0
NORM_EPS = 1e-6
ROWS = 512
MLP_ROWS = 256
LATE = 5
F32 = jnp.float32
BF16 = jnp.bfloat16
MESH = pl.DeviceIdType.MESH
VMEM_BYTES = 67_000_000


def rope_tables(rows, blocks, head_dim):
    half = head_dim // 2
    inv_freq = np.tile(ROPE_BASE ** (-2.0 * np.arange(half) / head_dim), 2)
    fine = np.arange(rows)[:, None] * inv_freq[None]
    coarse = np.arange(blocks)[:, None] * rows * inv_freq[None]
    return [f(a).astype(np.float32) for a in (fine, coarse) for f in (np.cos, np.sin)]


def send(src, dst, send_sem, recv_sem, peer):
    pltpu.make_async_remote_copy(src_ref=src, dst_ref=dst, send_sem=send_sem, recv_sem=recv_sem, device_id={'tp': peer}, device_id_type=MESH).start()


def wait_for(ref, sem):
    pltpu.make_async_copy(ref, ref, sem).wait()


def neighbours(tp_size):
    me = lax.axis_index('tp')
    chips = tp_size // 2
    chip, core = me // 2, me % 2
    right = ((chip + 1) % chips) * 2 + core
    left = ((chip + chips - 1) % chips) * 2 + core
    return me, chip, core, right, left, chip * 2 + 1 - core


ATT, PASS, PASS2, DONE1 = 2, 4, 5, 6
SUM_SLOTS, QK_SLOTS, WO_PIECES, WO_PASS, WO_PASS2 = 4, 3, 4, 5, 8


def attn_kernel(lens_ref, x_ref, wq_ref, wk_ref, wv_ref, g_ref, fcos_ref, fsin_ref, ccos_ref, csin_ref, wo_ref,
                o_ref, o_late, wo_all, kc_ref, vc_ref,
                q_s, k_s, kr_s, v_s, o_own, ss_own, ss_all, ss_send, ss_recv, o_send, o_loc, got_l, got_r, half_l, half_r, got_s, late_loc,
                pass_send, pass2_send, wo_send, wo_loc, wo_l, wo_r, wo_hl, wo_hr, wo_s, *, tp_size, chunks, blocks, width):
    s = pl.program_id(0)
    me, chip, core, right, left, sib = neighbours(tp_size)
    far = ((chip + 2) % (tp_size // 2)) * 2 + core
    rows = x_ref.shape[0]
    n = wq_ref.shape[1]
    heads = kc_ref.shape[1]
    mid = rows // 2
    wo_rows = wo_ref.shape[0]
    gathered = chunks - LATE

    def o_at(t, dev, off=0, size=rows):
        return o_ref.at[pl.ds(pl.multiple_of(t * rows + off, mid), size), pl.ds(pl.multiple_of(dev * n, n), n)]

    def wo_at(dev, off=0, size=wo_rows):
        return wo_all.at[pl.ds(pl.multiple_of(dev * wo_rows + off, wo_rows // WO_PIECES), size)]

    def send_wo(i):
        size = wo_rows // WO_PIECES
        piece = wo_ref.at[pl.ds(pl.multiple_of(i * size, size), size)]
        for peer, sem in ((right, wo_l), (left, wo_r), (sib, wo_s)):
            send(piece, wo_at(me, i * size, size), wo_send, sem, peer)

    def stage(lag, count=chunks):
        return pl.when((s >= lag) & (s < count + lag))

    @pl.when(s == 0)
    def _():
        barrier = pltpu.get_barrier_semaphore()
        for d in range(1, tp_size):
            pl.semaphore_signal(barrier, inc=1, device_id={'tp': (me + d) % tp_size}, device_id_type=MESH)
        pl.semaphore_wait(barrier, tp_size - 1)
        pltpu.make_async_copy(wo_ref, wo_at(me), wo_loc).start()

    @stage(PASS + LATE, gathered)
    def _():
        t = s - PASS - LATE
        slot = t % 8
        from_l, from_r = o_at(t, left), o_at(t, right)
        wait_for(from_l, got_l.at[slot])
        first = o_at(t, left, 0, mid)
        send(first, first, pass_send.at[slot], half_l.at[slot], right)
        send(from_l, from_l, pass_send.at[slot], got_s.at[slot], sib)
        wait_for(from_r, got_r.at[slot])
        second = o_at(t, right, mid, mid)
        send(second, second, pass_send.at[slot], half_r.at[slot], left)
        send(from_r, from_r, pass_send.at[slot], got_s.at[slot], sib)

    @stage(0)
    def _():
        x = x_ref[...]
        slot = s % QK_SLOTS
        b = (s // blocks) % 2
        here = pl.ds(pl.multiple_of((s % blocks) * rows, rows), rows)
        q = jnp.dot(x, wq_ref[...], preferred_element_type=F32)
        q_s[slot] = q
        k = jnp.dot(x, wk_ref[...], preferred_element_type=F32)
        k_s[slot] = k
        v = jnp.dot(x, wv_ref[...], preferred_element_type=F32).astype(BF16)
        for h in range(heads):
            vh = v[:, h * HEAD_DIM:(h + 1) * HEAD_DIM]
            vc_ref[0, h] = vh
            v_s[b, h, here, :] = vh
        qs = jnp.sum(q * q, axis=-1, keepdims=True)
        ks = jnp.sum(k * k, axis=-1, keepdims=True)
        lane = lax.broadcasted_iota(jnp.int32, (rows, 128), 1)
        t = jnp.transpose(jnp.where(lane < 64, qs, ks))
        ss_own[s % SUM_SLOTS] = jnp.concatenate([t[0:1], t[64:65]], axis=0)

    @stage(ATT)
    def _():
        t = s - ATT
        sslot = t % SUM_SLOTS
        for d in range(1, tp_size):
            peer = (me + d) % tp_size
            wait_for(ss_all.at[sslot, peer], ss_recv.at[sslot, peer])
        wait_for(ss_all.at[sslot, pl.ds(0, tp_size - 1)], ss_send.at[sslot])
        ss = ss_own[sslot]
        for d in range(1, tp_size):
            ss = ss + ss_all[sslot, (me + d) % tp_size]
        scale = lax.rsqrt(ss / width + NORM_EPS)
        col_scale = jnp.transpose(jnp.concatenate([scale, jnp.zeros((6, rows), F32)], axis=0))
        i = t % blocks
        b = t // blocks
        slot = t % 8
        lane = lax.broadcasted_iota(jnp.int32, (1, HEAD_DIM), 1)
        ccos, csin = ccos_ref[pl.ds(i, 1), :], csin_ref[pl.ds(i, 1), :]
        cos = fcos_ref[...] * ccos - fsin_ref[...] * csin
        sin = (fsin_ref[...] * ccos + fcos_ref[...] * csin) * jnp.where(lane < HEAD_DIM // 2, -1.0, 1.0)

        def rope(u):
            return (u * cos + pltpu.roll(u, HEAD_DIM // 2, axis=1) * sin).astype(BF16)

        length = lens_ref[b]
        qn = q_s[t % QK_SLOTS] * col_scale[:, 0:1] * g_ref[:, 0:n]
        kn = k_s[t % QK_SLOTS] * col_scale[:, 1:2] * g_ref[:, n:2 * n]
        qh = []
        for h in range(heads):
            sl = slice(h * HEAD_DIM, (h + 1) * HEAD_DIM)
            kr = rope(kn[:, sl])
            kc_ref[0, h] = kr
            kr_s[h, pl.ds(pl.multiple_of(i * rows, rows), rows), :] = kr
            qh.append(rope(qn[:, sl]))
        c = HEAD_DIM ** -0.5 * math.log2(math.e)
        for j in range(blocks):
            @pl.when(i == j)
            def _():
                kv = (j + 1) * rows
                col = lax.broadcasted_iota(jnp.int32, (1, kv), 1)
                bias = jnp.where(col < length, 0.0, -1e30).astype(F32)
                r = lax.broadcasted_iota(jnp.int32, (rows, rows), 0)
                cc = lax.broadcasted_iota(jnp.int32, (rows, rows), 1)
                tri = jnp.where(cc <= r, 0.0, -1e30).astype(F32)
                for h in range(heads):
                    sc = lax.dot_general(qh[h], kr_s[h, 0:kv, :], (((1,), (1,)), ((), ())), preferred_element_type=F32)
                    sc = sc + bias
                    diag = sc[:, j * rows:] + tri
                    sc = diag if j == 0 else jnp.concatenate([sc[:, :j * rows], diag], axis=1)
                    m = jnp.max(sc, axis=-1, keepdims=True)
                    e = jnp.exp2(sc * c - m * c)
                    p = (e * (1.0 / jnp.sum(e, axis=-1, keepdims=True))).astype(BF16)
                    o = jnp.dot(p, v_s[b % 2, h, 0:kv, :], preferred_element_type=F32)
                    o_own[slot, :, h * HEAD_DIM:(h + 1) * HEAD_DIM] = o.astype(BF16)

    @stage(PASS2 + LATE, gathered)
    def _():
        t = s - PASS2 - LATE
        slot = t % 8
        first, second = o_at(t, far, 0, mid), o_at(t, far, mid, mid)
        wait_for(first, half_l.at[slot])
        send(first, first, pass2_send.at[slot], got_s.at[slot], sib)
        wait_for(second, half_r.at[slot])
        send(second, second, pass2_send.at[slot], got_s.at[slot], sib)

    @stage(DONE1 + LATE, gathered)
    def _():
        t = s - DONE1 - LATE
        slot = t % 8
        part = o_ref.at[pl.ds(pl.multiple_of(t * rows, rows), rows)]
        wait_for(part.at[:, pl.ds(0, 3 * n)], o_send.at[slot])
        wait_for(part.at[:, pl.ds(0, n)], o_loc.at[slot])
        wait_for(part.at[:, pl.ds(0, 3 * n)], pass_send.at[slot])
        wait_for(part.at[:, pl.ds(0, n)], pass2_send.at[slot])
        wait_for(part.at[:, pl.ds(0, 4 * n)], got_s.at[slot])

    @stage(0)
    def _():
        slot = s % SUM_SLOTS
        for d in range(1, tp_size):
            send(ss_own.at[slot], ss_all.at[slot, me], ss_send.at[slot], ss_recv.at[slot, me], (me + d) % tp_size)

    @stage(ATT, LATE)
    def _():
        t = s - ATT
        pltpu.make_async_copy(o_own.at[t % 8], o_late.at[pl.ds(pl.multiple_of(t * rows, rows), rows)], late_loc.at[t]).start()

    @stage(DONE1, LATE)
    def _():
        t = s - DONE1
        wait_for(o_own.at[t % 8], late_loc.at[t])

    @stage(ATT + LATE, gathered)
    def _():
        t = s - ATT - LATE
        slot = t % 8
        own = o_own.at[(t + LATE) % 8]
        send(own, o_at(t, me), o_send.at[slot], got_l.at[slot], right)
        send(own, o_at(t, me), o_send.at[slot], got_r.at[slot], left)
        send(own, o_at(t, me), o_send.at[slot], got_s.at[slot], sib)
        pltpu.make_async_copy(own, o_at(t, me), o_loc.at[slot]).start()

    @pl.when(s < WO_PIECES)
    def _():
        send_wo(s)

    @pl.when(s == WO_PASS)
    def _():
        size = wo_rows // 2
        wait_for(wo_at(left), wo_l)
        send(wo_at(left, 0, size), wo_at(left, 0, size), wo_send, wo_hl, right)
        send(wo_at(left), wo_at(left), wo_send, wo_s, sib)
        wait_for(wo_at(right), wo_r)
        send(wo_at(right, size, size), wo_at(right, size, size), wo_send, wo_hr, left)
        send(wo_at(right), wo_at(right), wo_send, wo_s, sib)

    @pl.when(s == WO_PASS2)
    def _():
        size = wo_rows // 2
        wait_for(wo_at(far, 0, size), wo_hl)
        send(wo_at(far, 0, size), wo_at(far, 0, size), wo_send, wo_s, sib)
        wait_for(wo_at(far, size, size), wo_hr)
        send(wo_at(far, size, size), wo_at(far, size, size), wo_send, wo_s, sib)

    @pl.when(s == chunks + DONE1 - 1)
    def _():
        wait_for(wo_ref, wo_loc)
        wait_for(wo_all.at[pl.ds(0, 7 * wo_rows)], wo_send)
        wait_for(wo_all.at[pl.ds(0, 4 * wo_rows)], wo_s)


def attend(x, prompts, w_q, w_k, w_v, gains, lens, w_o, tp_size):
    total, d = x.shape
    n = w_q.shape[1]
    heads = n // HEAD_DIM
    seq = total // prompts
    blocks = seq // ROWS
    chunks = total // ROWS
    now = lambda s: jnp.minimum(s, chunks - 1)
    att = lambda s: jnp.clip(s - ATT, 0, chunks - 1)
    vmem = pl.BlockSpec(memory_space=pltpu.VMEM)
    hbm = pl.BlockSpec(memory_space=pl.ANY)
    dma = pltpu.SemaphoreType.DMA
    cache = jax.ShapeDtypeStruct((prompts, heads, seq, HEAD_DIM), BF16)
    tables = [jnp.asarray(t) for t in rope_tables(ROWS, blocks, HEAD_DIM)]
    return pl.pallas_call(
        functools.partial(attn_kernel, tp_size=tp_size, chunks=chunks, blocks=blocks, width=n * tp_size),
        grid=(chunks + DONE1,),
        in_specs=[
            pl.BlockSpec(memory_space=pltpu.SMEM),
            pl.BlockSpec((ROWS, d), lambda s: (now(s), 0)),
            vmem, vmem, vmem, vmem, vmem, vmem, vmem, vmem, hbm,
        ],
        out_specs=[
            hbm, hbm, hbm,
            pl.BlockSpec((1, heads, ROWS, HEAD_DIM), lambda s: (att(s) // blocks, 0, att(s) % blocks, 0)),
            pl.BlockSpec((1, heads, ROWS, HEAD_DIM), lambda s: (now(s) // blocks, 0, now(s) % blocks, 0)),
        ],
        out_shape=[
            jax.ShapeDtypeStruct((total - LATE * ROWS, n * tp_size), BF16),
            jax.ShapeDtypeStruct((LATE * ROWS, n), BF16),
            jax.ShapeDtypeStruct((w_o.shape[0] * tp_size, w_o.shape[1]), BF16),
            cache, cache,
        ],
        scratch_shapes=[
            pltpu.VMEM((QK_SLOTS, ROWS, n), F32),
            pltpu.VMEM((QK_SLOTS, ROWS, n), F32),
            pltpu.VMEM((heads, seq, HEAD_DIM), BF16),
            pltpu.VMEM((2, heads, seq, HEAD_DIM), BF16),
            pltpu.VMEM((8, ROWS, n), BF16),
            pltpu.VMEM((SUM_SLOTS, 2, ROWS), F32),
            pltpu.VMEM((SUM_SLOTS, tp_size, 2, ROWS), F32),
            dma((SUM_SLOTS,)), dma((SUM_SLOTS, tp_size)),
            dma((8,)), dma((8,)), dma((8,)), dma((8,)), dma((8,)), dma((8,)), dma((8,)), dma((LATE,)), dma((8,)), dma((8,)),
            dma, dma, dma, dma, dma, dma, dma,
        ],
        compiler_params=pltpu.CompilerParams(collective_id=1, has_side_effects=True, vmem_limit_bytes=VMEM_BYTES),
        cost_estimate=pl.CostEstimate(flops=6 * total * d * n, bytes_accessed=4 * total * d, transcendentals=0),
        name="attend",
    )(lens, x, w_q, w_k, w_v, gains, *tables, w_o)


ADD, MERGE, FINAL, RELAY, RELAY2, DONE = 1, 3, 5, 7, 9, 10
LATE_PASS, LATE_PASS2, LATE_DONE = 3, 5, 14
SIB_SLOTS, C_SLOTS = 3, 6


def mlp_kernel(o_ref, late_ref, x_ref, wo_in, g_ref, wg_in, wu_in, wd_in, y_ref, wo_ref, wg_ref, wu_ref, wd_ref, o_late, o_s, h_ref, act_s, m_s, c_s, r_sib, r1_l, r1_r, r2_l, r2_r, h_own, y_own,
               sib_send, sib_recv, s1_send, r1_lsem, r1_rsem, s2_send, r2_lsem, r2_rsem,
               y_send, y_loc, y_l, y_r, yh_l, yh_r, yf_send, yh_send, y_sib, free_s, late_send, late_loc, late_l, late_r, late_hl, late_hr, late_s, w_sem, *, tp_size, chunks, early):
    s = pl.program_id(0)
    me, chip, core, right, left, sib = neighbours(tp_size)
    chips = tp_size // 2
    rows, d = x_ref.shape
    n, late_mid = late_ref.shape[1], late_ref.shape[0] // 2
    g_at = g_ref.shape[1] - 2 * d
    half = rows // 2
    piece = half // chips
    sub = piece // 2
    opp = (chip + 2) % chips
    rchip = (chip + 1) % chips
    lchip = (chip + chips - 1) % chips
    own = pl.ds(pl.multiple_of(core * half, half), half)
    other = pl.ds(pl.multiple_of((1 - core) * half, half), half)

    def at(p, off=0, size=piece):
        return pl.ds(pl.multiple_of(p * piece + off, sub), size)

    def y_rows(t, c, p, off=0, size=piece):
        return y_ref.at[pl.ds(pl.multiple_of((t + chunks - early) % chunks * rows + c * half + p * piece + off, sub), size)]

    def late(dev, off=0, size=2 * late_mid):
        return o_late.at[pl.ds(off, size), pl.ds(pl.multiple_of(dev * n, n), n)]

    def stage(lag):
        return pl.when((s >= lag) & (s < chunks + lag))

    @pl.when(s == 0)
    def _():
        loads = [pltpu.make_async_copy(src, dst, w_sem.at[i]) for i, (src, dst) in enumerate(
            ((wo_in, wo_ref), (wg_in, wg_ref), (wu_in, wu_ref), (wd_in, wd_ref)))]
        for load in loads:
            load.start()
        barrier = pltpu.get_barrier_semaphore()
        for peer in (right, left, sib):
            pl.semaphore_signal(barrier, inc=1, device_id={'tp': peer}, device_id_type=MESH)
        pl.semaphore_wait(barrier, 3)
        for peer, sem in ((right, late_l), (left, late_r), (sib, late_s)):
            send(late_ref, late(me), late_send, sem, peer)
        pltpu.make_async_copy(late_ref, late(me), late_loc).start()
        for load in loads:
            load.wait()

    @pl.when(s == LATE_PASS)
    def _():
        wait_for(late(left), late_l)
        send(late(left, 0, late_mid), late(left, 0, late_mid), late_send, late_hl, right)
        send(late(left), late(left), late_send, late_s, sib)
        wait_for(late(right), late_r)
        send(late(right, late_mid, late_mid), late(right, late_mid, late_mid), late_send, late_hr, left)
        send(late(right), late(right), late_send, late_s, sib)

    @pl.when(s == LATE_PASS2)
    def _():
        far = opp * 2 + core
        wait_for(late(far, 0, late_mid), late_hl)
        send(late(far, 0, late_mid), late(far, 0, late_mid), late_send, late_s, sib)
        wait_for(late(far, late_mid, late_mid), late_hr)
        send(late(far, late_mid, late_mid), late(far, late_mid, late_mid), late_send, late_s, sib)

    @pl.when(s == LATE_DONE)
    def _():
        wait_for(late_ref, late_loc)
        wait_for(o_late.at[:, pl.ds(0, 7 * n)], late_send)
        wait_for(o_late.at[:, pl.ds(0, 4 * n)], late_s)

    @pl.when(s < early)
    def _():
        o_s[...] = o_ref[...]

    @pl.when((s >= early) & (s < chunks))
    def _():
        o_s[...] = o_late[pl.ds(pl.multiple_of((s - early) * rows, rows), rows), :]

    @stage(0)
    def _():
        f = act_s.shape[1]
        o = o_s[...]
        sq = jnp.zeros((rows, 1), F32)
        for lo in range(0, d, 512):
            a = jnp.dot(o, wo_ref[:, lo:lo + 512], preferred_element_type=F32).astype(BF16)
            h_ref[:, lo:lo + 512] = a
            a = a.astype(F32)
            sq = sq + jnp.sum(a * a, axis=-1, keepdims=True)
        scale = lax.rsqrt(sq / d + NORM_EPS)
        for lo in range(0, d, 512):
            a = h_ref[:, lo:lo + 512].astype(F32)
            h_ref[:, lo:lo + 512] = (x_ref[:, lo:lo + 512].astype(F32) + a * scale * g_ref[:, g_at + lo:g_at + lo + 512]).astype(BF16)
        h = h_ref[...]
        for lo in range(0, f, 512):
            gate = jnp.dot(h, wg_ref[:, lo:lo + 512], preferred_element_type=F32)
            up = jnp.dot(h, wu_ref[:, lo:lo + 512], preferred_element_type=F32)
            act_s[:, lo:lo + 512] = (jax.nn.silu(gate) * up).astype(BF16)
        act = act_s[...]
        for lo in range(0, d, 512):
            m_s[s % SIB_SLOTS, :, lo:lo + 512] = jnp.dot(act, wd_ref[:, lo:lo + 512], preferred_element_type=F32).astype(BF16)
        h_own[s % 8] = h_ref[pl.ds(pl.multiple_of(core * half + chip * piece, piece), piece), :]

    @stage(ADD)
    def _():
        t = s - ADD
        slot, ms, cs = t % 8, t % SIB_SLOTS, t % C_SLOTS
        wait_for(r_sib.at[ms], sib_recv.at[ms])
        wait_for(m_s.at[ms, other], sib_send.at[ms])
        c_s[cs] = (m_s[ms, own, :].astype(F32) + r_sib[ms].astype(F32)).astype(BF16)

        @pl.when(t < chunks - SIB_SLOTS)
        def _():
            pl.semaphore_signal(free_s, inc=1, device_id={'tp': sib}, device_id_type=MESH)

    @stage(MERGE)
    def _():
        slot, cs = (s - MERGE) % 8, (s - MERGE) % C_SLOTS
        wait_for(r1_l.at[slot], r1_lsem.at[slot])
        c_s[cs, at(rchip, 0, sub), :] = (c_s[cs, at(rchip, 0, sub), :].astype(F32) + r1_l[slot].astype(F32)).astype(BF16)
        wait_for(r1_r.at[slot], r1_rsem.at[slot])
        c_s[cs, at(lchip, sub, sub), :] = (c_s[cs, at(lchip, sub, sub), :].astype(F32) + r1_r[slot].astype(F32)).astype(BF16)

    @stage(FINAL)
    def _():
        t = s - FINAL
        slot, cs = t % 8, t % C_SLOTS
        wait_for(r2_l.at[slot], r2_lsem.at[slot])
        wait_for(r2_r.at[slot], r2_rsem.at[slot])
        wait_for(c_s.at[cs, pl.ds(0, piece)], s1_send.at[slot])
        wait_for(c_s.at[cs, pl.ds(0, 2 * piece)], s2_send.at[slot])
        m = c_s[cs, at(chip), :].astype(F32) + r2_l[slot].astype(F32) + r2_r[slot].astype(F32)
        m = m.astype(BF16).astype(F32)
        scale = lax.rsqrt(jnp.sum(m * m, axis=-1, keepdims=True) / d + NORM_EPS)
        y_own[slot] = (h_own[slot].astype(F32) + m * scale * g_ref[:, g_at + d:]).astype(BF16)

    @stage(RELAY)
    def _():
        t = s - RELAY
        slot = t % 8
        from_l, from_r = y_rows(t, core, lchip), y_rows(t, core, rchip)
        wait_for(from_l, y_l.at[slot])
        first = y_rows(t, core, lchip, 0, sub)
        send(first, first, yf_send.at[slot], yh_l.at[slot], right)
        send(from_l, from_l, yf_send.at[slot], y_sib.at[t], sib)
        wait_for(from_r, y_r.at[slot])
        second = y_rows(t, core, rchip, sub, sub)
        send(second, second, yf_send.at[slot], yh_r.at[slot], left)
        send(from_r, from_r, yf_send.at[slot], y_sib.at[t], sib)

    @stage(RELAY2)
    def _():
        t = s - RELAY2
        slot = t % 8
        first, second = y_rows(t, core, opp, 0, sub), y_rows(t, core, opp, sub, sub)
        wait_for(first, yh_l.at[slot])
        send(first, first, yh_send.at[slot], y_sib.at[t], sib)
        wait_for(second, yh_r.at[slot])
        send(second, second, yh_send.at[slot], y_sib.at[t], sib)

    @stage(DONE)
    def _():
        t = s - DONE
        slot = t % 8
        base = pl.multiple_of(t * rows, rows)
        wait_for(y_ref.at[pl.ds(base, piece)], y_loc.at[slot])
        wait_for(y_ref.at[pl.ds(base, 3 * piece)], y_send.at[slot])
        wait_for(y_ref.at[pl.ds(base, 3 * piece)], yf_send.at[slot])
        wait_for(y_ref.at[pl.ds(base, piece)], yh_send.at[slot])
        wait_for(y_ref.at[pl.ds(base, chips * piece)], y_sib.at[t])

    @stage(FINAL)
    def _():
        t = s - FINAL
        slot = t % 8
        dst = y_rows(t, core, chip)
        send(y_own.at[slot], dst, y_send.at[slot], y_l.at[slot], right)
        send(y_own.at[slot], dst, y_send.at[slot], y_r.at[slot], left)
        send(y_own.at[slot], dst, y_send.at[slot], y_sib.at[t], sib)
        pltpu.make_async_copy(y_own.at[slot], dst, y_loc.at[slot]).start()

    @stage(MERGE)
    def _():
        slot, cs = (s - MERGE) % 8, (s - MERGE) % C_SLOTS
        send(c_s.at[cs, at(rchip)], r2_l.at[slot], s2_send.at[slot], r2_lsem.at[slot], right)
        send(c_s.at[cs, at(lchip)], r2_r.at[slot], s2_send.at[slot], r2_rsem.at[slot], left)

    @stage(ADD)
    def _():
        slot, cs = (s - ADD) % 8, (s - ADD) % C_SLOTS
        send(c_s.at[cs, at(opp, 0, sub)], r1_l.at[slot], s1_send.at[slot], r1_lsem.at[slot], right)
        send(c_s.at[cs, at(opp, sub, sub)], r1_r.at[slot], s1_send.at[slot], r1_rsem.at[slot], left)

    @stage(0)
    def _():
        @pl.when(s >= SIB_SLOTS)
        def _():
            pl.semaphore_wait(free_s, 1)

        ms = s % SIB_SLOTS
        send(m_s.at[ms, other], r_sib.at[ms], sib_send.at[ms], sib_recv.at[ms], sib)


def mlp(o, late, x, w_o, gains, w_gate, w_up, w_down, tp_size):
    total, d = x.shape
    f = w_gate.shape[1]
    chunks = total // MLP_ROWS
    half = MLP_ROWS // 2
    piece = half // (tp_size // 2)
    sub = piece // 2
    early = o.shape[0] // MLP_ROWS
    front = pl.BlockSpec((MLP_ROWS, d), lambda s: (jnp.minimum(s, early - 1), 0))
    chunk = pl.BlockSpec((MLP_ROWS, d), lambda s: ((jnp.minimum(s, chunks - 1) + chunks - early) % chunks, 0))
    vmem = pl.BlockSpec(memory_space=pltpu.VMEM)
    hbm = pl.BlockSpec(memory_space=pl.ANY)
    dma = pltpu.SemaphoreType.DMA
    return pl.pallas_call(
        functools.partial(mlp_kernel, tp_size=tp_size, chunks=chunks, early=early),
        grid=(chunks + DONE,),
        in_specs=[front, hbm, chunk, hbm, vmem, hbm, hbm, hbm],
        out_specs=hbm,
        out_shape=jax.ShapeDtypeStruct((total, d), BF16),
        scratch_shapes=[
            pltpu.VMEM(w_o.shape, BF16), pltpu.VMEM(w_gate.shape, BF16), pltpu.VMEM(w_up.shape, BF16), pltpu.VMEM(w_down.shape, BF16),
            pltpu.VMEM((late.shape[0], d), BF16),
            pltpu.VMEM((MLP_ROWS, d), BF16),
            pltpu.VMEM((MLP_ROWS, d), BF16),
            pltpu.VMEM((MLP_ROWS, f), BF16),
            pltpu.VMEM((SIB_SLOTS, MLP_ROWS, d), BF16),
            pltpu.VMEM((C_SLOTS, half, d), BF16),
            pltpu.VMEM((SIB_SLOTS, half, d), BF16),
            pltpu.VMEM((8, sub, d), BF16), pltpu.VMEM((8, sub, d), BF16),
            pltpu.VMEM((8, piece, d), BF16), pltpu.VMEM((8, piece, d), BF16),
            pltpu.VMEM((8, piece, d), BF16), pltpu.VMEM((8, piece, d), BF16),
            dma((SIB_SLOTS,)), dma((SIB_SLOTS,)),
            dma((8,)), dma((8,)), dma((8,)), dma((8,)), dma((8,)), dma((8,)),
            dma((8,)), dma((8,)), dma((8,)), dma((8,)), dma((8,)), dma((8,)), dma((8,)), dma((8,)),
            dma((chunks,)),
            pltpu.SemaphoreType.REGULAR,
            dma, dma, dma, dma, dma, dma, dma, dma((4,)),
        ],
        compiler_params=pltpu.CompilerParams(collective_id=2, has_side_effects=True, vmem_limit_bytes=VMEM_BYTES),
        cost_estimate=pl.CostEstimate(flops=6 * total * d * f + 2 * total * d * d, bytes_accessed=4 * total * d, transcendentals=0),
        name="mlp",
    )(o, late, x, w_o, gains, w_gate, w_up, w_down)


def solution(mesh):
    tp_size = mesh.shape['tp']

    def local_layer(tokens, seq_lens, w_q, w_k, w_v, w_o, g_q, g_k, g_attn, g_mlp, w_gate, w_up, w_down):
        prompts, seq, d = tokens.shape
        x = tokens.reshape(prompts * seq, d)
        gains = jnp.concatenate([g_q, g_k, g_attn, g_mlp]).astype(F32)[None]
        o, o_late, w_o_full, k_cache, v_cache = attend(x, prompts, w_q, w_k, w_v, gains, seq_lens, w_o, tp_size)
        y = mlp(o, o_late, x, w_o_full, gains, w_gate, w_up, w_down, tp_size)
        return y.reshape(prompts, seq, d), k_cache, v_cache

    return jax.shard_map(local_layer, mesh=mesh, in_specs=(P('dp', None, None), P('dp'), P(None, 'tp'), P(None, 'tp'), P(None, 'tp'), P('tp', None), P('tp'), P('tp'), P(), P(), P(None, 'tp'), P(None, 'tp'), P('tp', None)), out_specs=(P('dp', None, None), P('dp', 'tp', None, None), P('dp', 'tp', None, None)), check_vma=False)
```
